32 devices in a mesh: group: 2 (over y), ctx: 4 (over z), head: 4 (over x, core).
Axes of the slice: x: 2, y: 2, z: 4, core: 2. Of those that a mesh axis runs over, the one named last changes fastest.
Arguments:
- query_nope: bfloat16 [512, 8192], P(('group', 'ctx'), 'head'), parts along dimension 0, may hold values from -6 to 6
- query_rope: bfloat16 [512, 4096], P(('group', 'ctx'), 'head'), parts along dimension 0, may hold values from -16 to 16
- kv_latent: bfloat16 [512, 512], P(('group', 'ctx'), 'head'), parts along dimension 0, may hold values from -1300 to 1300
- key_rope: bfloat16 [512, 64], P(('group', 'ctx')), parts along dimension 0, may hold values from -16 to 16
- latent_gain: float32 [512], replicated, may hold values from 0.1 to 1.9
- w_key: bfloat16 [512, 8192], P(None, 'head'), may hold values from -0.25 to 0.25
- w_value: bfloat16 [512, 8192], P(None, 'head'), may hold values from -0.25 to 0.25
- block_order: int32 [16], P('group'), parts along dimension 0, may hold values from 0 to 7, as said below
Outputs:
- attention_out: bfloat16 [512, 8192], P(('group', 'ctx'), 'head'), parts along dimension 0
The draws below stay inside these ranges and needn't reach their ends.
There are 2 independent parts, one for each index of `group`. The reference program is written for one: setup_inputs(seed, part) draws one part's arguments, and reference() takes and returns one part's arrays. A program takes and returns all parts, laid end to end along the dimension named above; an argument that names none is the same for every part. Nothing has to cross between parts.
Inputs may be any that keep to these rules, and one draw needn't show every extreme that they name: `block_order`: A permutation of 0 to 7. Entries 2 c and 2 c + 1, for each c < 4, add up to 7.
All inputs are finite; a program needn't handle non-finite values.
Results may differ from the reference program's by a relative error of at most 0.0081.
Values may be sent and summed in bfloat16 or wider, within the bound.
A program may use at most 64 MiB of HBM per device.

```python
import jax
import jax.numpy as jnp
from jax import lax

LATENT = 512
ROPE = 64
NOPE = 128
VALUE_DIM = 128
HEADS = 64
TOK_DEV = 64
TOKENS = 256
BLOCK = 32


def draw_query_rope(key, part):
    values = jnp.clip(jax.random.normal(jax.random.fold_in(key, 22), (TOKENS, HEADS, ROPE), jnp.float32), -6.0, 6.0)
    return values.reshape(TOKENS, HEADS * ROPE).astype(jnp.bfloat16)


def draw_key_rope(key, part):
    values = jnp.clip(jax.random.normal(jax.random.fold_in(key, 32), (TOKENS, ROPE), jnp.float32), -6.0, 6.0)
    return values.astype(jnp.bfloat16)


def draw_kv_latent(key, part):
    row_scale = jnp.exp(jax.random.uniform(jax.random.fold_in(key, 41), (TOKENS, 1), jnp.float32, 0.0, jnp.log(10.0)))
    column_scale = jnp.exp(jax.random.uniform(jax.random.fold_in(key, 42), (1, LATENT), jnp.float32, 0.0, jnp.log(10.0)))
    column_scale = column_scale * jnp.exp(jnp.log(3.0) * jnp.arange(LATENT, dtype=jnp.float32)[None, :] / LATENT)
    noise = jnp.clip(jax.random.normal(jax.random.fold_in(key, 45), (TOKENS, LATENT), jnp.float32), -4.0, 4.0)
    return (noise * row_scale * column_scale).astype(jnp.bfloat16)


def draw_block_order(key, part):
    devices = TOKENS // TOK_DEV
    blocks = 2 * devices
    shuffled = jax.random.permutation(jax.random.fold_in(key, 51), devices).astype(jnp.int32)
    flipped = jax.random.randint(jax.random.fold_in(key, 52), (devices,), 0, 2).astype(jnp.int32)
    early = jnp.where(flipped == 1, blocks - 1 - shuffled, shuffled)
    late = blocks - 1 - early
    return jnp.stack([early, late], 1).reshape(blocks).astype(jnp.int32)


def block_scale(key, extent, shards, smallest, top_value):
    def one(axis_at, blocks):
        steps = jax.random.uniform(jax.random.fold_in(jax.random.fold_in(key, 6), axis_at), (blocks,), jnp.float32, smallest / len(shards), top_value / len(shards))
        return jnp.repeat(jnp.exp(steps), extent[axis_at] // blocks).reshape((-1,) + (1,) * (len(extent) - axis_at - 1))

    factor_of = one(*shards[0])
    for cut in shards[1:]:
        factor_of = factor_of * one(*cut)
    return factor_of


def scatter_about(rng, extent, deviation, bound, shards=(), kind=jnp.bfloat16):
    result = jax.random.normal(rng, extent, jnp.float32) * deviation
    if len(shards) > 0:
        result = block_scale(rng, extent, shards, -0.22, 0.18) * result
    return jnp.clip(result, min=-bound, max=bound).astype(kind)


def setup_inputs(seed: int = 0, part: int = 0) -> dict:
    arg_keys = jax.random.split(jax.random.key(seed), 9)
    part_splits = jax.random.split(jax.random.fold_in(arg_keys[8], part), 9)
    return {
        "query_nope": scatter_about(part_splits[0], (TOKENS, HEADS * NOPE), 1.0, 6.0, ((0, 4), (1, 4))),
        "query_rope": draw_query_rope(jax.random.fold_in(jax.random.fold_in(arg_keys[8], part), 71), part),
        "kv_latent": draw_kv_latent(jax.random.fold_in(jax.random.fold_in(arg_keys[8], part), 71), part),
        "key_rope": draw_key_rope(jax.random.fold_in(jax.random.fold_in(arg_keys[8], part), 71), part),
        "latent_gain": jnp.clip(1.0 + 0.18 * jax.random.normal(arg_keys[4], (LATENT,), jnp.float32), 0.1, 1.9),
        "w_key": scatter_about(arg_keys[5], (LATENT, HEADS * NOPE), LATENT ** -0.5, 0.25, ((1, 4),)),
        "w_value": scatter_about(arg_keys[6], (LATENT, HEADS * VALUE_DIM), LATENT ** -0.5, 0.25, ((1, 4),)),
        "block_order": draw_block_order(jax.random.fold_in(jax.random.fold_in(arg_keys[8], part), 71), part),
    }


EPSILON = 1e-06

def rope_angle(positions, width):
    half_width = width // 2
    frequency = jnp.exp(-jnp.log(10000.0) * jnp.arange(half_width, dtype=jnp.float32) / half_width)
    return positions.astype(jnp.float32)[:, None] * frequency[None, :]

def rotate_pairs(values, angle):
    half_width = values.shape[-1] // 2
    first_half = values[..., :half_width]
    second = values[..., half_width:]
    cosine = jnp.cos(angle)
    sine_part = jnp.sin(angle)
    return jnp.concatenate([first_half * cosine - second * sine_part, second * cosine + first_half * sine_part], -1)

def reference(query_nope, query_rope, kv_latent, key_rope, latent_gain, w_key, w_value, block_order):
    row_ids = jnp.arange(TOKENS, dtype=jnp.int32)
    position = (block_order[row_ids // BLOCK] * BLOCK + row_ids % BLOCK).astype(jnp.int32)
    latent = kv_latent.astype(jnp.float32)
    mean_square = lax.optimization_barrier(jnp.mean(latent * latent, axis=1, keepdims=True))
    normed = (latent * lax.rsqrt(mean_square + EPSILON) * latent_gain[None, :]).astype(jnp.bfloat16)
    key_angle = rope_angle(position, ROPE)
    key_rotated = rotate_pairs(key_rope.astype(jnp.float32), key_angle).astype(jnp.bfloat16)
    query_rotated = rotate_pairs(query_rope.astype(jnp.float32).reshape(TOKENS, HEADS, ROPE), key_angle[:, None, :]).astype(jnp.bfloat16)
    nope_heads = jnp.transpose(query_nope.reshape(TOKENS, HEADS, NOPE), (1, 0, 2))
    rope_heads = jnp.transpose(query_rotated, (1, 0, 2))
    key_heads = jnp.transpose(w_key.reshape(LATENT, HEADS, NOPE), (1, 0, 2))
    value_heads = jnp.transpose(w_value.reshape(LATENT, HEADS, VALUE_DIM), (1, 0, 2))
    visible = position[None, :] <= position[:, None]
    score_scale = 1.0 / (NOPE + ROPE) ** 0.5

    def one_head(operands):
        nope_part, rope_part, key_map, value_map = operands
        absorbed = lax.dot_general(nope_part, key_map, (((1,), (1,)), ((), ())), preferred_element_type=jnp.float32).astype(jnp.bfloat16)
        scores = jnp.dot(absorbed, normed.T, preferred_element_type=jnp.float32)
        scores = (scores + jnp.dot(rope_part, key_rotated.T, preferred_element_type=jnp.float32)) * score_scale
        scores = jnp.where(visible, scores, -jnp.inf)
        row_max = lax.optimization_barrier(jnp.max(scores, axis=1, keepdims=True))
        exps = jnp.where(visible, jnp.exp(scores - row_max), 0.0)
        row_total = lax.optimization_barrier(jnp.sum(exps, axis=1, keepdims=True))
        mixed = (jnp.dot(exps.astype(jnp.bfloat16), normed, preferred_element_type=jnp.float32) / row_total).astype(jnp.bfloat16)
        return jnp.dot(mixed, value_map, preferred_element_type=jnp.float32)
    per_head = lax.map(one_head, (nope_heads, rope_heads, key_heads, value_heads))
    return jnp.transpose(per_head, (1, 0, 2)).reshape(TOKENS, HEADS * VALUE_DIM).astype(jnp.bfloat16)
```

```python
from functools import partial
import math

import jax
import jax.numpy as jnp
from jax import lax
from jax.experimental import pallas as pl
from jax.experimental.pallas import tpu as pltpu
from jax.sharding import PartitionSpec as P

ROPE = 64
NOPE = 128
VALUE_DIM = 128


EPSILON = 1e-06
NEGATIVE = -1e30


def rope_angle(positions, width):
    half_width = width // 2
    frequency = jnp.exp(-jnp.log(10000.0) * jnp.arange(half_width, dtype=jnp.float32) / half_width)
    return positions.astype(jnp.float32)[:, None] * frequency[None, :]


def rotate_pairs(values, angle):
    half_width = values.shape[-1] // 2
    first_half = values[..., :half_width]
    second = values[..., half_width:]
    cosine = jnp.cos(angle)
    sine_part = jnp.sin(angle)
    return jnp.concatenate(
        [first_half * cosine - second * sine_part, second * cosine + first_half * sine_part], -1
    )


def block_positions(begin_row, row_count, table, block_rows):
    row_ids = begin_row + jnp.arange(row_count, dtype=jnp.int32)
    blocks = row_ids // block_rows
    slot_ids = jnp.arange(table.shape[0], dtype=jnp.int32)
    looked = jnp.sum(jnp.where(blocks[:, None] == slot_ids[None, :], table[None, :], 0), axis=1)
    return looked * block_rows + row_ids % block_rows


def block_length(row_count, shard_rows):
    best_rows = shard_rows
    for factor in range(1, row_count // shard_rows + 1):
        if row_count // shard_rows % factor == 0 and shard_rows * factor <= max(512, shard_rows):
            best_rows = shard_rows * factor
    return best_rows


def attend_block(
    carried,
    query_latent,
    query_rotated,
    query_place,
    key_latent,
    key_rotated,
    key_place,
    score_scale,
):
    running_max, running_total, summed = carried
    contract = (((1,), (1,)), ((), ()))
    scores = lax.dot_general(query_latent, key_latent, contract, preferred_element_type=jnp.float32)
    scores = (
        scores
        + lax.dot_general(query_rotated, key_rotated, contract, preferred_element_type=jnp.float32)
    ) * score_scale
    visible = key_place[None, :] <= query_place[:, None]
    scores = jnp.where(visible, scores, NEGATIVE)
    new_max = jnp.maximum(running_max, jnp.max(scores, axis=1))
    exps = jnp.where(visible, jnp.exp(scores - new_max[:, None]), 0.0)
    shrink = jnp.exp(running_max - new_max)
    running_total = running_total * shrink + jnp.sum(exps, axis=1)
    summed = summed * shrink[:, None] + jnp.dot(
        exps.astype(jnp.bfloat16), key_latent, preferred_element_type=jnp.float32
    )
    return (new_max, running_total, summed)


def per_device(
    query_nope, query_rope, kv_latent, key_rope, latent_gain, w_key, w_value, block_order
):
    tokens_here = query_nope.shape[0]
    heads_here = w_key.shape[1] // NOPE
    latent_width = w_key.shape[0]
    block_rows = tokens_here // 2
    score_scale = 1.0 / math.sqrt(NOPE + ROPE)
    first_row = lax.axis_index("ctx") * tokens_here
    query_place = block_positions(first_row, tokens_here, block_order, block_rows)
    query_angle = rope_angle(query_place, ROPE)
    query_rotated = rotate_pairs(
        query_rope.astype(jnp.float32).reshape(tokens_here, heads_here, ROPE),
        query_angle[:, None, :],
    )
    query_rotated = query_rotated.astype(jnp.bfloat16).reshape(tokens_here * heads_here, ROPE)
    absorbed = jnp.einsum(
        "thd,lhd->thl",
        query_nope.reshape(tokens_here, heads_here, NOPE),
        w_key.reshape(latent_width, heads_here, NOPE),
        preferred_element_type=jnp.float32,
    )
    absorbed = absorbed.astype(jnp.bfloat16).reshape(tokens_here * heads_here, latent_width)
    row_place = jnp.repeat(query_place, heads_here)
    groups = ((absorbed, query_rotated, row_place),)
    initial = tuple(
        (
            (
                jnp.full((member[0].shape[0],), NEGATIVE, jnp.float32),
                jnp.zeros((member[0].shape[0],), jnp.float32),
                jnp.zeros((member[0].shape[0], latent_width), jnp.float32),
            )
            for member in groups
        )
    )
    columns = kv_latent.shape[1]
    column_part = kv_latent.astype(jnp.float32)
    square = lax.psum(jnp.sum(column_part * column_part, axis=1), "head")
    gain_part = lax.dynamic_slice_in_dim(latent_gain, lax.axis_index("head") * columns, columns, 0)
    scaled = (
        column_part * lax.rsqrt(square / latent_width + EPSILON)[:, None] * gain_part[None, :]
    ).astype(jnp.bfloat16)
    normed = lax.all_gather(scaled, "head", axis=1, tiled=True)
    key_rotated = rotate_pairs(key_rope.astype(jnp.float32), query_angle).astype(jnp.bfloat16)
    key_latent = lax.all_gather(normed, "ctx", axis=0, tiled=True)
    make_key_rotated = lax.all_gather(key_rotated, "ctx", axis=0, tiled=True)
    row_count = key_latent.shape[0]
    length = block_length(row_count, tokens_here)
    block_count = row_count // length
    latent_blocks = key_latent.reshape(block_count, length, latent_width)
    rotated_blocks = make_key_rotated.reshape(block_count, length, ROPE)
    block_starts = length * jnp.arange(block_count, dtype=jnp.int32)

    def one_block(state_now, operands):
        latent_block, rotated_block, first_key = operands
        key_place = block_positions(first_key, length, block_order, block_rows)
        updated = []
        for member, member_state in zip(groups, state_now):
            advance = partial(
                attend_block,
                query_latent=member[0],
                query_rotated=member[1],
                query_place=member[2],
                key_latent=latent_block,
                key_rotated=rotated_block,
                key_place=key_place,
                score_scale=score_scale,
            )
            updated.append(advance(member_state))
        return (tuple(updated), None)

    result, unused = lax.scan(one_block, initial, (latent_blocks, rotated_blocks, block_starts))
    mixed = jnp.concatenate(
        [
            (member_state[2] / member_state[1][:, None]).astype(jnp.bfloat16)
            for member_state in result
        ],
        0,
    )
    mixed = mixed.reshape(tokens_here, heads_here, latent_width)
    output = jnp.einsum(
        "thl,lhe->the",
        mixed,
        w_value.reshape(latent_width, heads_here, VALUE_DIM),
        preferred_element_type=jnp.float32,
    )
    return output.astype(jnp.bfloat16).reshape(tokens_here, heads_here * VALUE_DIM)


LANES = 128
FUSED_ROWS = 512
HEAD_GROUP = 4
MESH = pl.DeviceIdType.MESH


def flip(index, stride):
    return index + stride - 2 * stride * ((index // stride) % 2)


def strides_of(count):
    strides = []
    stride = count // 2
    while stride >= 1:
        strides.append(stride)
        stride //= 2
    return strides


def lane_frequency(lanes):
    half = ROPE // 2
    rest = lanes % half
    frequency = jnp.ones(lanes.shape, jnp.float32)
    bit = 1
    while bit < half:
        frequency = frequency * jnp.where((rest // bit) % 2 == 1, 10000.0 ** (-bit / half), 1.0)
        bit *= 2
    return frequency


def turn(values, cosine, signed_sine, first_lanes):
    half = ROPE // 2
    ahead = pltpu.roll(values, LANES - half, 1)
    behind = pltpu.roll(values, half, 1)
    return values * cosine + jnp.where(first_lanes, ahead, behind) * signed_sine


def fused_kernel(
    contexts,
    shards,
    order_ref,
    gain_ref,
    nope_hbm,
    rope_hbm,
    latent_hbm,
    key_rope_hbm,
    w_key_hbm,
    w_value_hbm,
    out_hbm,
    nope,
    rope,
    w_key,
    w_value,
    latents,
    ropes,
    queries,
    keys,
    outs,
    load_sem,
    key_sem,
    own_sem,
    out_sem,
    latent_send,
    latent_recv,
    rope_send,
    rope_recv,
):
    group = lax.axis_index("group")
    ctx = lax.axis_index("ctx")
    shard = lax.axis_index("head")
    tokens = nope.shape[0]
    heads = nope.shape[1] // NOPE
    latent_width = w_key.shape[0]
    block_rows = tokens // 2
    blocks = 2 * contexts
    rope_rows = ropes.shape[2]
    chunks = key_sem.shape[0]
    chunk = w_key.shape[1] // chunks

    own_latent = pltpu.make_async_copy(latent_hbm, latents.at[ctx, shard], own_sem.at[0])
    own_rope = pltpu.make_async_copy(
        key_rope_hbm.at[pl.ds(pl.multiple_of(shard * rope_rows, rope_rows), rope_rows), :],
        ropes.at[ctx, shard],
        own_sem.at[1],
    )
    own_latent.start()
    own_rope.start()
    load_nope = pltpu.make_async_copy(nope_hbm, nope, load_sem.at[0])
    load_rope = pltpu.make_async_copy(rope_hbm, rope, load_sem.at[1])
    load_value = pltpu.make_async_copy(w_value_hbm, w_value, load_sem.at[2])
    load_nope.start()
    load_keys = []
    for part in range(chunks):
        columns = pl.ds(part * chunk, chunk)
        load = pltpu.make_async_copy(w_key_hbm.at[:, columns], w_key.at[:, columns], key_sem.at[part])
        load.start()
        load_keys.append(load)
    load_rope.start()
    load_value.start()

    peers = [(group, flip_all(ctx, step), shard) for step in range(1, contexts)]
    strides = strides_of(shards)
    partners = [(group, ctx, flip(shard, stride)) for stride in strides]
    barrier = pltpu.get_barrier_semaphore()
    for device in peers + partners:
        pl.semaphore_signal(barrier, inc=1, device_id=device, device_id_type=MESH)
    pl.semaphore_wait(barrier, len(peers) + len(partners))

    own_latent.wait()
    own_rope.wait()
    sent = []

    def send(slot, index, target):
        place, part = slot
        for buffer, send_sem, recv_sem in (
            (latents, latent_send, latent_recv),
            (ropes, rope_send, rope_recv),
        ):
            copy = pltpu.make_async_remote_copy(
                src_ref=buffer.at[place, part],
                dst_ref=buffer.at[place, part],
                send_sem=send_sem.at[index],
                recv_sem=recv_sem.at[place, part],
                device_id=target,
                device_id_type=MESH,
            )
            copy.start()
            sent.append(copy)

    def arrive(place, part):
        for buffer, send_sem, recv_sem in (
            (latents, latent_send, latent_recv),
            (ropes, rope_send, rope_recv),
        ):
            pltpu.make_async_remote_copy(
                src_ref=buffer.at[place, part],
                dst_ref=buffer.at[place, part],
                send_sem=send_sem.at[0],
                recv_sem=recv_sem.at[place, part],
                device_id=partners[0] if partners else peers[0],
                device_id_type=MESH,
            ).wait_recv()

    counter = [0]

    def next_index():
        counter[0] += 1
        return counter[0] - 1

    for target in peers:
        send((ctx, shard), next_index(), target)
    for target in partners:
        send((ctx, shard), next_index(), target)

    def absorb(part):
        load_keys[part].wait()
        for head in range(part * heads // chunks, (part + 1) * heads // chunks):
            columns = slice(head * NOPE, (head + 1) * NOPE)
            absorbed = lax.dot_general(
                nope[:, columns],
                w_key[:, columns],
                (((1,), (1,)), ((), ())),
                preferred_element_type=jnp.float32,
            )
            queries[head * tokens : (head + 1) * tokens, :latent_width] = absorbed.astype(jnp.bfloat16)

    load_nope.wait()
    absorb(0)

    lanes = lax.broadcasted_iota(jnp.int32, (1, LANES), 1)
    frequency = lane_frequency(lanes)
    first_lanes = lanes % ROPE < ROPE // 2
    sign = jnp.where(first_lanes, -1.0, 1.0)
    table_rows = -(-(blocks + 2) // 8) * 8
    row_ids = lax.broadcasted_iota(jnp.int32, (table_rows, LANES), 0)
    base = jnp.zeros((table_rows, LANES), jnp.int32)
    slots = [order_ref[slot] for slot in range(blocks)] + [order_ref[2 * ctx], order_ref[2 * ctx + 1]]
    for row, slot in enumerate(slots):
        base = jnp.where(row_ids == row, slot * block_rows, base)
    base_angle = base.astype(jnp.float32) * frequency
    step_angle = (
        lax.broadcasted_iota(jnp.int32, (block_rows, LANES), 0).astype(jnp.float32) * frequency
    )
    base_cos, base_sin = jnp.cos(base_angle), jnp.sin(base_angle)
    step_cos, step_sin = jnp.cos(step_angle), jnp.sin(step_angle)

    def tables(first, second):
        cosines, sines = [], []
        for row in (first, second):
            one_cos, one_sin = base_cos[row : row + 1], base_sin[row : row + 1]
            cosines.append(one_cos * step_cos - one_sin * step_sin)
            sines.append((one_sin * step_cos + one_cos * step_sin) * sign)
        return jnp.concatenate(cosines, 0), jnp.concatenate(sines, 0)

    query_cos, query_sin = tables(blocks, blocks + 1)
    per_tile = LANES // ROPE
    load_rope.wait()
    for tile in range(heads // per_tile):
        turned = turn(
            rope[:, tile * LANES : (tile + 1) * LANES].astype(jnp.float32),
            query_cos,
            query_sin,
            first_lanes,
        )
        for inner in range(per_tile):
            head = tile * per_tile + inner
            queries[head * tokens : (head + 1) * tokens, latent_width:] = jnp.where(
                lanes // ROPE == inner, turned, 0.0
            ).astype(jnp.bfloat16)

    steps = list(range(1, contexts))
    for order, step in enumerate(steps):
        if order + 1 < chunks:
            absorb(order + 1)
        place = flip_all(ctx, step)
        arrive(place, shard)
        for target in partners:
            send((place, shard), next_index(), target)
    for part in range(len(steps) + 1, chunks):
        absorb(part)

    held = [shard]
    for level, stride in enumerate(strides):
        fresh = [flip(part, stride) for part in held]
        for step in range(contexts):
            place = ctx if step == 0 else flip_all(ctx, step)
            for part in fresh:
                arrive(place, part)
                for target in partners[level + 1 :]:
                    send((place, part), next_index(), target)
        held = held + fresh

    gain = gain_ref[...]
    for place in range(contexts):
        raw = jnp.concatenate([latents[place, part] for part in range(shards)], 1).astype(jnp.float32)
        mean = jnp.sum(raw * raw, axis=1, keepdims=True) / latent_width
        normed = raw * lax.rsqrt(mean + EPSILON) * gain
        rows = slice(place * tokens, (place + 1) * tokens)
        keys[rows, :latent_width] = normed.astype(jnp.bfloat16)
        key_raw = jnp.concatenate([ropes[place, part] for part in range(shards)], 0).astype(jnp.float32)
        key_raw = jnp.concatenate([key_raw] * per_tile, 1)
        key_cos, key_sin = tables(2 * place, 2 * place + 1)
        keys[rows, latent_width:] = turn(key_raw, key_cos, key_sin, first_lanes).astype(jnp.bfloat16)

    total_rows = contexts * tokens
    key_ids = lax.broadcasted_iota(jnp.int32, (1, total_rows), 1)
    key_base = jnp.zeros((1, total_rows), jnp.int32)
    for row in range(blocks):
        key_base = jnp.where(key_ids // block_rows == row, slots[row], key_base)
    key_place = key_base * block_rows + key_ids % block_rows
    query_ids = lax.broadcasted_iota(jnp.int32, (HEAD_GROUP * tokens, 1), 0) % tokens
    query_place = (
        jnp.where(query_ids // block_rows == 0, slots[blocks], slots[blocks + 1]) * block_rows
        + query_ids % block_rows
    )
    visible = key_place <= query_place
    exponent = math.log2(math.e) / math.sqrt(NOPE + ROPE)

    load_value.wait()
    stores = []
    for cluster in range(heads // HEAD_GROUP):
        rows = slice(cluster * HEAD_GROUP * tokens, (cluster + 1) * HEAD_GROUP * tokens)
        scores = lax.dot_general(
            queries[rows, :], keys[...], (((1,), (1,)), ((), ())), preferred_element_type=jnp.float32
        )
        scores = jnp.where(visible, scores, NEGATIVE)
        top = jnp.max(scores, axis=1, keepdims=True)
        exps = jnp.exp2((scores - top) * exponent)
        total = jnp.sum(exps, axis=1, keepdims=True)
        mixed = jnp.dot(
            exps.astype(jnp.bfloat16), keys[:, :latent_width], preferred_element_type=jnp.float32
        )
        mixed = (mixed * (1.0 / total)).astype(jnp.bfloat16)
        for inner in range(HEAD_GROUP):
            head = cluster * HEAD_GROUP + inner
            columns = slice(head * VALUE_DIM, (head + 1) * VALUE_DIM)
            outs[:, columns] = jnp.dot(
                mixed[inner * tokens : (inner + 1) * tokens],
                w_value[:, columns],
                preferred_element_type=jnp.float32,
            ).astype(jnp.bfloat16)
        columns = pl.ds(cluster * HEAD_GROUP * VALUE_DIM, HEAD_GROUP * VALUE_DIM)
        store = pltpu.make_async_copy(outs.at[:, columns], out_hbm.at[:, columns], out_sem.at[cluster])
        store.start()
        stores.append(store)
    for store in stores:
        store.wait()
    for copy in sent:
        copy.wait_send()


def flip_all(index, step):
    result = index
    bit = 1
    while bit <= step:
        if (step // bit) % 2 == 1:
            result = flip(result, bit)
        bit *= 2
    return result


def fused_device(
    contexts,
    shards,
    query_nope,
    query_rope,
    kv_latent,
    key_rope,
    latent_gain,
    w_key,
    w_value,
    block_order,
):
    tokens, nope_width = query_nope.shape
    heads = nope_width // NOPE
    latent_width = w_key.shape[0]
    rope_rows = tokens // shards
    sends = (contexts - 1) + contexts * (shards - 1)
    anywhere = pl.BlockSpec(memory_space=pl.ANY)
    return pl.pallas_call(
        partial(fused_kernel, contexts, shards),
        out_shape=jax.ShapeDtypeStruct((tokens, heads * VALUE_DIM), jnp.bfloat16),
        in_specs=[
            pl.BlockSpec(memory_space=pltpu.SMEM),
            pl.BlockSpec(memory_space=pltpu.VMEM),
        ]
        + [anywhere] * 6,
        out_specs=anywhere,
        scratch_shapes=[
            pltpu.VMEM(query_nope.shape, jnp.bfloat16),
            pltpu.VMEM(query_rope.shape, jnp.bfloat16),
            pltpu.VMEM(w_key.shape, jnp.bfloat16),
            pltpu.VMEM(w_value.shape, jnp.bfloat16),
            pltpu.VMEM((contexts, shards) + kv_latent.shape, jnp.bfloat16),
            pltpu.VMEM((contexts, shards, rope_rows, ROPE), jnp.bfloat16),
            pltpu.VMEM((heads * tokens, latent_width + LANES), jnp.bfloat16),
            pltpu.VMEM((contexts * tokens, latent_width + LANES), jnp.bfloat16),
            pltpu.VMEM((tokens, heads * VALUE_DIM), jnp.bfloat16),
            pltpu.SemaphoreType.DMA((3,)),
            pltpu.SemaphoreType.DMA((4,)),
            pltpu.SemaphoreType.DMA((2,)),
            pltpu.SemaphoreType.DMA((heads // HEAD_GROUP,)),
            pltpu.SemaphoreType.DMA((sends,)),
            pltpu.SemaphoreType.DMA((contexts, shards)),
            pltpu.SemaphoreType.DMA((sends,)),
            pltpu.SemaphoreType.DMA((contexts, shards)),
        ],
        compiler_params=pltpu.CompilerParams(collective_id=0, has_side_effects=True),
    )(
        block_order,
        latent_gain.reshape(1, latent_width),
        query_nope,
        query_rope,
        kv_latent,
        key_rope,
        w_key,
        w_value,
    )


def power_of_two(count):
    return count & (count - 1) == 0


def solution(mesh):
    contexts, shards = mesh.shape["ctx"], mesh.shape["head"]

    def device_step(*arguments):
        small = contexts * arguments[0].shape[0] <= FUSED_ROWS
        if small and power_of_two(contexts) and power_of_two(shards):
            return fused_device(contexts, shards, *arguments)
        return per_device(*arguments)

    return jax.shard_map(
        device_step,
        mesh=mesh,
        in_specs=(
            P(("group", "ctx"), "head"),
            P(("group", "ctx"), "head"),
            P(("group", "ctx"), "head"),
            P(("group", "ctx"), None),
            P(),
            P(None, "head"),
            P(None, "head"),
            P("group"),
        ),
        out_specs=P(("group", "ctx"), "head"),
        check_vma=False,
    )
```

```python
from functools import partial
import math

import jax
import jax.numpy as jnp
from jax import lax
from jax.experimental import pallas as pl
from jax.experimental.pallas import tpu as pltpu
from jax.sharding import PartitionSpec as P

ROPE = 64
NOPE = 128
VALUE_DIM = 128


EPSILON = 1e-06
NEGATIVE = -1e30


def rope_angle(positions, width):
    half_width = width // 2
    frequency = jnp.exp(-jnp.log(10000.0) * jnp.arange(half_width, dtype=jnp.float32) / half_width)
    return positions.astype(jnp.float32)[:, None] * frequency[None, :]


def rotate_pairs(values, angle):
    half_width = values.shape[-1] // 2
    first_half = values[..., :half_width]
    second = values[..., half_width:]
    cosine = jnp.cos(angle)
    sine_part = jnp.sin(angle)
    return jnp.concatenate(
        [first_half * cosine - second * sine_part, second * cosine + first_half * sine_part], -1
    )


def block_positions(begin_row, row_count, table, block_rows):
    row_ids = begin_row + jnp.arange(row_count, dtype=jnp.int32)
    blocks = row_ids // block_rows
    slot_ids = jnp.arange(table.shape[0], dtype=jnp.int32)
    looked = jnp.sum(jnp.where(blocks[:, None] == slot_ids[None, :], table[None, :], 0), axis=1)
    return looked * block_rows + row_ids % block_rows


def block_length(row_count, shard_rows):
    best_rows = shard_rows
    for factor in range(1, row_count // shard_rows + 1):
        if row_count // shard_rows % factor == 0 and shard_rows * factor <= max(512, shard_rows):
            best_rows = shard_rows * factor
    return best_rows


def attend_block(
    carried,
    query_latent,
    query_rotated,
    query_place,
    key_latent,
    key_rotated,
    key_place,
    score_scale,
):
    running_max, running_total, summed = carried
    contract = (((1,), (1,)), ((), ()))
    scores = lax.dot_general(query_latent, key_latent, contract, preferred_element_type=jnp.float32)
    scores = (
        scores
        + lax.dot_general(query_rotated, key_rotated, contract, preferred_element_type=jnp.float32)
    ) * score_scale
    visible = key_place[None, :] <= query_place[:, None]
    scores = jnp.where(visible, scores, NEGATIVE)
    new_max = jnp.maximum(running_max, jnp.max(scores, axis=1))
    exps = jnp.where(visible, jnp.exp(scores - new_max[:, None]), 0.0)
    shrink = jnp.exp(running_max - new_max)
    running_total = running_total * shrink + jnp.sum(exps, axis=1)
    summed = summed * shrink[:, None] + jnp.dot(
        exps.astype(jnp.bfloat16), key_latent, preferred_element_type=jnp.float32
    )
    return (new_max, running_total, summed)


def per_device(
    query_nope, query_rope, kv_latent, key_rope, latent_gain, w_key, w_value, block_order
):
    tokens_here = query_nope.shape[0]
    heads_here = w_key.shape[1] // NOPE
    latent_width = w_key.shape[0]
    block_rows = tokens_here // 2
    score_scale = 1.0 / math.sqrt(NOPE + ROPE)
    first_row = lax.axis_index("ctx") * tokens_here
    query_place = block_positions(first_row, tokens_here, block_order, block_rows)
    query_angle = rope_angle(query_place, ROPE)
    query_rotated = rotate_pairs(
        query_rope.astype(jnp.float32).reshape(tokens_here, heads_here, ROPE),
        query_angle[:, None, :],
    )
    query_rotated = query_rotated.astype(jnp.bfloat16).reshape(tokens_here * heads_here, ROPE)
    absorbed = jnp.einsum(
        "thd,lhd->thl",
        query_nope.reshape(tokens_here, heads_here, NOPE),
        w_key.reshape(latent_width, heads_here, NOPE),
        preferred_element_type=jnp.float32,
    )
    absorbed = absorbed.astype(jnp.bfloat16).reshape(tokens_here * heads_here, latent_width)
    row_place = jnp.repeat(query_place, heads_here)
    groups = ((absorbed, query_rotated, row_place),)
    initial = tuple(
        (
            (
                jnp.full((member[0].shape[0],), NEGATIVE, jnp.float32),
                jnp.zeros((member[0].shape[0],), jnp.float32),
                jnp.zeros((member[0].shape[0], latent_width), jnp.float32),
            )
            for member in groups
        )
    )
    columns = kv_latent.shape[1]
    column_part = kv_latent.astype(jnp.float32)
    square = lax.psum(jnp.sum(column_part * column_part, axis=1), "head")
    gain_part = lax.dynamic_slice_in_dim(latent_gain, lax.axis_index("head") * columns, columns, 0)
    scaled = (
        column_part * lax.rsqrt(square / latent_width + EPSILON)[:, None] * gain_part[None, :]
    ).astype(jnp.bfloat16)
    normed = lax.all_gather(scaled, "head", axis=1, tiled=True)
    key_rotated = rotate_pairs(key_rope.astype(jnp.float32), query_angle).astype(jnp.bfloat16)
    key_latent = lax.all_gather(normed, "ctx", axis=0, tiled=True)
    make_key_rotated = lax.all_gather(key_rotated, "ctx", axis=0, tiled=True)
    row_count = key_latent.shape[0]
    length = block_length(row_count, tokens_here)
    block_count = row_count // length
    latent_blocks = key_latent.reshape(block_count, length, latent_width)
    rotated_blocks = make_key_rotated.reshape(block_count, length, ROPE)
    block_starts = length * jnp.arange(block_count, dtype=jnp.int32)

    def one_block(state_now, operands):
        latent_block, rotated_block, first_key = operands
        key_place = block_positions(first_key, length, block_order, block_rows)
        updated = []
        for member, member_state in zip(groups, state_now):
            advance = partial(
                attend_block,
                query_latent=member[0],
                query_rotated=member[1],
                query_place=member[2],
                key_latent=latent_block,
                key_rotated=rotated_block,
                key_place=key_place,
                score_scale=score_scale,
            )
            updated.append(advance(member_state))
        return (tuple(updated), None)

    result, unused = lax.scan(one_block, initial, (latent_blocks, rotated_blocks, block_starts))
    mixed = jnp.concatenate(
        [
            (member_state[2] / member_state[1][:, None]).astype(jnp.bfloat16)
            for member_state in result
        ],
        0,
    )
    mixed = mixed.reshape(tokens_here, heads_here, latent_width)
    output = jnp.einsum(
        "thl,lhe->the",
        mixed,
        w_value.reshape(latent_width, heads_here, VALUE_DIM),
        preferred_element_type=jnp.float32,
    )
    return output.astype(jnp.bfloat16).reshape(tokens_here, heads_here * VALUE_DIM)


LANES = 128
FUSED_ROWS = 512
HEAD_GROUP = 4
VMEM_BYTES = 67043328
VMEM_SPARE = 2**17
VMEM_GRANT = 24 * 2**20
MESH = pl.DeviceIdType.MESH


def flip(index, stride):
    return index + stride - 2 * stride * ((index // stride) % 2)


def strides_of(count):
    strides = []
    stride = count // 2
    while stride >= 1:
        strides.append(stride)
        stride //= 2
    return strides


def lane_frequency(lanes):
    half = ROPE // 2
    rest = lanes % half
    frequency = jnp.ones(lanes.shape, jnp.float32)
    bit = 1
    while bit < half:
        frequency = frequency * jnp.where((rest // bit) % 2 == 1, 10000.0 ** (-bit / half), 1.0)
        bit *= 2
    return frequency


def turn(values, cosine, signed_sine, first_lanes):
    half = ROPE // 2
    ahead = pltpu.roll(values, LANES - half, 1)
    behind = pltpu.roll(values, half, 1)
    return values * cosine + jnp.where(first_lanes, ahead, behind) * signed_sine


def fused_kernel(
    contexts,
    shards,
    order_hbm,
    gain_hbm,
    nope_hbm,
    rope_hbm,
    latent_hbm,
    key_rope_hbm,
    w_key_hbm,
    w_value_hbm,
    queries,
    keys,
    bias,
    w_value,
    order_ref,
    gain_ref,
    nope,
    rope,
    w_key,
    latents,
    ropes,
    load_sem,
    key_sem,
    own_sem,
    latent_send,
    latent_recv,
    rope_send,
    rope_recv,
):
    group = lax.axis_index("group")
    ctx = lax.axis_index("ctx")
    shard = lax.axis_index("head")
    tokens = nope.shape[0]
    heads = nope.shape[1] // NOPE
    latent_width = w_key.shape[0]
    block_rows = tokens // 2
    blocks = 2 * contexts
    rope_rows = ropes.shape[2]
    chunks = key_sem.shape[0]
    chunk = w_key.shape[1] // chunks

    peers = [(group, flip_all(ctx, step), shard) for step in range(contexts - 1, 0, -1)]
    strides = strides_of(shards)
    partners = [(group, ctx, flip(shard, stride)) for stride in strides]
    barrier = pltpu.get_barrier_semaphore()
    for device in peers + partners:
        pl.semaphore_signal(barrier, inc=1, device_id=device, device_id_type=MESH)
    own_latent = pltpu.make_async_copy(latent_hbm, latents.at[ctx, shard], own_sem.at[0])
    own_rope = pltpu.make_async_copy(
        key_rope_hbm.at[pl.ds(pl.multiple_of(shard * rope_rows, rope_rows), rope_rows), :],
        ropes.at[ctx, shard],
        own_sem.at[1],
    )
    own_latent.start()
    own_rope.start()
    load_order = pltpu.make_async_copy(order_hbm, order_ref, own_sem.at[2])
    load_gain = pltpu.make_async_copy(gain_hbm, gain_ref, own_sem.at[3])
    load_nope = pltpu.make_async_copy(nope_hbm, nope, load_sem.at[0])
    load_rope = pltpu.make_async_copy(rope_hbm, rope, load_sem.at[1])
    load_value = pltpu.make_async_copy(w_value_hbm, w_value, load_sem.at[2])
    load_nope.start()
    load_keys = []
    for part in range(chunks):
        columns = pl.ds(part * chunk, chunk)
        load = pltpu.make_async_copy(w_key_hbm.at[:, columns], w_key.at[:, columns], key_sem.at[part])
        load.start()
        load_keys.append(load)
    load_rope.start()
    load_order.start()
    load_gain.start()
    load_value.start()

    pl.semaphore_wait(barrier, len(peers) + len(partners))

    own_latent.wait()
    own_rope.wait()
    sent = []

    def send(slot, index, target):
        place, part = slot
        for buffer, send_sem, recv_sem in (
            (latents, latent_send, latent_recv),
            (ropes, rope_send, rope_recv),
        ):
            copy = pltpu.make_async_remote_copy(
                src_ref=buffer.at[place, part],
                dst_ref=buffer.at[place, part],
                send_sem=send_sem.at[index],
                recv_sem=recv_sem.at[place, part],
                device_id=target,
                device_id_type=MESH,
            )
            copy.start()
            sent.append(copy)

    def arrive(place, part):
        for buffer, send_sem, recv_sem in (
            (latents, latent_send, latent_recv),
            (ropes, rope_send, rope_recv),
        ):
            pltpu.make_async_remote_copy(
                src_ref=buffer.at[place, part],
                dst_ref=buffer.at[place, part],
                send_sem=send_sem.at[0],
                recv_sem=recv_sem.at[place, part],
                device_id=partners[0] if partners else peers[0],
                device_id_type=MESH,
            ).wait_recv()

    counter = [0]

    def next_index():
        counter[0] += 1
        return counter[0] - 1

    for target in peers:
        send((ctx, shard), next_index(), target)
    for target in partners:
        send((ctx, shard), next_index(), target)

    def absorb(part):
        load_keys[part].wait()
        for head in range(part * heads // chunks, (part + 1) * heads // chunks):
            columns = slice(head * NOPE, (head + 1) * NOPE)
            absorbed = lax.dot_general(
                nope[:, columns],
                w_key[:, columns],
                (((1,), (1,)), ((), ())),
                preferred_element_type=jnp.float32,
            )
            queries[head * tokens : (head + 1) * tokens, :latent_width] = absorbed.astype(jnp.bfloat16)

    load_nope.wait()
    absorb(0)
    load_order.wait()
    load_gain.wait()

    lanes = lax.broadcasted_iota(jnp.int32, (1, LANES), 1)
    frequency = lane_frequency(lanes)
    first_lanes = lanes % ROPE < ROPE // 2
    sign = jnp.where(first_lanes, -1.0, 1.0)
    table_rows = -(-(blocks + 2) // 8) * 8
    row_ids = lax.broadcasted_iota(jnp.int32, (table_rows, LANES), 0)
    base = jnp.zeros((table_rows, LANES), jnp.int32)
    slots = [order_ref[slot] for slot in range(blocks)] + [order_ref[2 * ctx], order_ref[2 * ctx + 1]]
    for row, slot in enumerate(slots):
        base = jnp.where(row_ids == row, slot * block_rows, base)
    base_angle = base.astype(jnp.float32) * frequency
    step_angle = (
        lax.broadcasted_iota(jnp.int32, (block_rows, LANES), 0).astype(jnp.float32) * frequency
    )
    base_cos, base_sin = jnp.cos(base_angle), jnp.sin(base_angle)
    step_cos, step_sin = jnp.cos(step_angle), jnp.sin(step_angle)

    def tables(first, second):
        cosines, sines = [], []
        for row in (first, second):
            one_cos, one_sin = base_cos[row : row + 1], base_sin[row : row + 1]
            cosines.append(one_cos * step_cos - one_sin * step_sin)
            sines.append((one_sin * step_cos + one_cos * step_sin) * sign)
        return jnp.concatenate(cosines, 0), jnp.concatenate(sines, 0)

    query_cos, query_sin = tables(blocks, blocks + 1)
    per_tile = LANES // ROPE
    load_rope.wait()
    for tile in range(heads // per_tile):
        turned = turn(
            rope[:, tile * LANES : (tile + 1) * LANES].astype(jnp.float32),
            query_cos,
            query_sin,
            first_lanes,
        )
        for inner in range(per_tile):
            head = tile * per_tile + inner
            queries[head * tokens : (head + 1) * tokens, latent_width:] = jnp.where(
                lanes // ROPE == inner, turned, 0.0
            ).astype(jnp.bfloat16)

    steps = list(range(1, contexts))
    for order, step in enumerate(steps):
        if order + 1 < chunks:
            absorb(order + 1)
        place = flip_all(ctx, step)
        arrive(place, shard)
        for target in partners:
            send((place, shard), next_index(), target)
    for part in range(len(steps) + 1, chunks):
        absorb(part)

    held = [shard]
    for level, stride in enumerate(strides):
        fresh = [flip(part, stride) for part in held]
        for step in range(contexts):
            place = ctx if step == 0 else flip_all(ctx, step)
            for part in fresh:
                arrive(place, part)
                for target in partners[level + 1 :]:
                    send((place, part), next_index(), target)
        held = held + fresh

    gain = gain_ref[...]
    for place in range(contexts):
        raw = jnp.concatenate([latents[place, part] for part in range(shards)], 1).astype(jnp.float32)
        mean = jnp.sum(raw * raw, axis=1, keepdims=True) / latent_width
        normed = raw * lax.rsqrt(mean + EPSILON) * gain
        rows = slice(place * tokens, (place + 1) * tokens)
        keys[rows, :latent_width] = normed.astype(jnp.bfloat16)
        key_raw = jnp.concatenate([ropes[place, part] for part in range(shards)], 0).astype(jnp.float32)
        key_raw = jnp.concatenate([key_raw] * per_tile, 1)
        key_cos, key_sin = tables(2 * place, 2 * place + 1)
        keys[rows, latent_width:] = turn(key_raw, key_cos, key_sin, first_lanes).astype(jnp.bfloat16)

    total_rows = contexts * tokens
    key_ids = lax.broadcasted_iota(jnp.int32, (1, total_rows), 1)
    key_base = jnp.zeros((1, total_rows), jnp.int32)
    for row in range(blocks):
        key_base = jnp.where(key_ids // block_rows == row, slots[row], key_base)
    key_place = key_base * block_rows + key_ids % block_rows
    query_ids = lax.broadcasted_iota(jnp.int32, (tokens, 1), 0)
    query_place = (
        jnp.where(query_ids // block_rows == 0, slots[blocks], slots[blocks + 1]) * block_rows
        + query_ids % block_rows
    )
    bias[...] = jnp.where(key_place <= query_place, 0.0, NEGATIVE)
    load_value.wait()
    for copy in sent:
        copy.wait_send()


def attend_kernel(queries, keys, bias, w_value, out_hbm, outs, out_sem):
    tokens = bias.shape[0]
    heads = queries.shape[0] // tokens
    latent_width = w_value.shape[0]
    exponent = math.log2(math.e) / math.sqrt(NOPE + ROPE)
    hidden = jnp.concatenate([bias[...]] * HEAD_GROUP, 0)
    stores = []
    for cluster in range(heads // HEAD_GROUP):
        rows = slice(cluster * HEAD_GROUP * tokens, (cluster + 1) * HEAD_GROUP * tokens)
        scores = lax.dot_general(
            queries[rows, :], keys[...], (((1,), (1,)), ((), ())), preferred_element_type=jnp.float32
        )
        scores = scores + hidden
        top = jnp.max(scores, axis=1, keepdims=True)
        exps = jnp.exp2((scores - top) * exponent)
        total = jnp.sum(exps, axis=1, keepdims=True)
        mixed = jnp.dot(
            exps.astype(jnp.bfloat16), keys[:, :latent_width], preferred_element_type=jnp.float32
        )
        mixed = (mixed * (1.0 / total)).astype(jnp.bfloat16)
        for inner in range(HEAD_GROUP):
            head = cluster * HEAD_GROUP + inner
            columns = slice(head * VALUE_DIM, (head + 1) * VALUE_DIM)
            outs[:, columns] = jnp.dot(
                mixed[inner * tokens : (inner + 1) * tokens],
                w_value[:, columns],
                preferred_element_type=jnp.float32,
            ).astype(jnp.bfloat16)
        columns = pl.ds(cluster * HEAD_GROUP * VALUE_DIM, HEAD_GROUP * VALUE_DIM)
        store = pltpu.make_async_copy(outs.at[:, columns], out_hbm.at[:, columns], out_sem.at[cluster])
        store.start()
        stores.append(store)
    for store in stores:
        store.wait()


def flip_all(index, step):
    result = index
    bit = 1
    while bit <= step:
        if (step // bit) % 2 == 1:
            result = flip(result, bit)
        bit *= 2
    return result


def fused_device(
    contexts,
    shards,
    query_nope,
    query_rope,
    kv_latent,
    key_rope,
    latent_gain,
    w_key,
    w_value,
    block_order,
):
    tokens, nope_width = query_nope.shape
    heads = nope_width // NOPE
    latent_width = w_key.shape[0]
    rope_rows = tokens // shards
    sends = (contexts - 1) + contexts * (shards - 1)
    anywhere = pl.BlockSpec(memory_space=pl.ANY)
    on_chip = pl.BlockSpec(memory_space=pltpu.VMEM)
    rows = contexts * tokens
    handed = 2 * (heads * tokens + rows) * (latent_width + LANES) + 4 * tokens * rows + 2 * w_value.size
    prepared = pl.pallas_call(
        partial(fused_kernel, contexts, shards),
        out_shape=[
            pltpu.VMEM((heads * tokens, latent_width + LANES), jnp.bfloat16),
            pltpu.VMEM((rows, latent_width + LANES), jnp.bfloat16),
            pltpu.VMEM((tokens, rows), jnp.float32),
            pltpu.VMEM(w_value.shape, jnp.bfloat16),
        ],
        in_specs=[anywhere] * 8,
        out_specs=[on_chip] * 4,
        scratch_shapes=[
            pltpu.SMEM(block_order.shape, jnp.int32),
            pltpu.VMEM((1, latent_width), jnp.float32),
            pltpu.VMEM(query_nope.shape, jnp.bfloat16),
            pltpu.VMEM(query_rope.shape, jnp.bfloat16),
            pltpu.VMEM(w_key.shape, jnp.bfloat16),
            pltpu.VMEM((contexts, shards) + kv_latent.shape, jnp.bfloat16),
            pltpu.VMEM((contexts, shards, rope_rows, ROPE), jnp.bfloat16),
            pltpu.SemaphoreType.DMA((3,)),
            pltpu.SemaphoreType.DMA((4,)),
            pltpu.SemaphoreType.DMA((4,)),
            pltpu.SemaphoreType.DMA((sends,)),
            pltpu.SemaphoreType.DMA((contexts, shards)),
            pltpu.SemaphoreType.DMA((sends,)),
            pltpu.SemaphoreType.DMA((contexts, shards)),
        ],
        compiler_params=pltpu.CompilerParams(
            collective_id=0,
            has_side_effects=True,
            vmem_limit_bytes=VMEM_BYTES - VMEM_SPARE - handed,
        ),
    )(
        block_order,
        latent_gain.reshape(1, latent_width),
        query_nope,
        query_rope,
        kv_latent,
        key_rope,
        w_key,
        w_value,
    )
    return pl.pallas_call(
        attend_kernel,
        out_shape=jax.ShapeDtypeStruct((tokens, heads * VALUE_DIM), jnp.bfloat16),
        in_specs=[on_chip] * 4,
        out_specs=anywhere,
        scratch_shapes=[
            pltpu.VMEM((tokens, heads * VALUE_DIM), jnp.bfloat16),
            pltpu.SemaphoreType.DMA((heads // HEAD_GROUP,)),
        ],
        compiler_params=pltpu.CompilerParams(vmem_limit_bytes=VMEM_GRANT),
    )(*prepared)


def power_of_two(count):
    return count & (count - 1) == 0


def solution(mesh):
    contexts, shards = mesh.shape["ctx"], mesh.shape["head"]

    def device_step(*arguments):
        small = contexts * arguments[0].shape[0] <= FUSED_ROWS
        if small and power_of_two(contexts) and power_of_two(shards):
            return fused_device(contexts, shards, *arguments)
        return per_device(*arguments)

    return jax.shard_map(
        device_step,
        mesh=mesh,
        in_specs=(
            P(("group", "ctx"), "head"),
            P(("group", "ctx"), "head"),
            P(("group", "ctx"), "head"),
            P(("group", "ctx"), None),
            P(),
            P(None, "head"),
            P(None, "head"),
            P("group"),
        ),
        out_specs=P(("group", "ctx"), "head"),
        check_vma=False,
    )
```
